128 devices in a mesh: seq: 16 (over x_lo, z, core), head: 4 (over y), batch: 2 (over x_hi).
Axes of the slice: x: 4 (x_hi: 2, x_lo: 2; x = x_hi * 2 + x_lo), y: 4, z: 4, core: 2. Of those that a mesh axis runs over, the one named last changes fastest.
Arguments:
- tokens: bfloat16 [32768, 2048], P(('batch', 'seq')), parts along dimension 0, may hold values from -6 to 6
- neighbor_bank: bfloat16 [512, 256, 2048], P(('batch', 'seq')), parts along dimension 0, may hold values from -2100 to 2100
- slots: int32 [512], P(('batch', 'seq')), parts along dimension 0, may hold values from 0 to 15
- w_query: bfloat16 [2048, 2048], P('seq', 'head'), may hold values from -0.125 to 0.125
- w_key: bfloat16 [2048, 2048], P('seq', 'head'), may hold values from -0.125 to 0.125
- w_value: bfloat16 [2048, 2048], P('seq', 'head'), may hold values from -0.125 to 0.125
- w_out: bfloat16 [2048, 2048], P('head', 'seq'), may hold values from -0.125 to 0.125
Outputs:
- cross_out: bfloat16 [32768, 2048], P(('batch', 'seq'), 'head'), parts along dimension 0
The draws below stay inside these ranges and needn't reach their ends.
There are 2 independent parts, one for each index of `batch`. The reference program is written for one: setup_inputs(seed, part) draws one part's arguments, and reference() takes and returns one part's arrays. A program takes and returns all parts, laid end to end along the dimension named above; an argument that names none is the same for every part. Nothing has to cross between parts.
Inputs may be any that keep to these rules, and one draw needn't show every extreme that they name: Entry c picks row c // 16 * 16 + slots[c] of neighbor_bank.
All inputs are finite; a program needn't handle non-finite values.
Results may differ from the reference program's by a relative error of at most 0.006.
The reference program's roundings to bfloat16 on the way (of `normed`, `queries`, `retrieved`, `weights` and `attended`) count: a program that leaves them out, or rounds other values in their place, can miss the bound.
Values may be sent and summed in bfloat16 or wider, within the bound.
No kernel may reach another device: no remote copies, remote signals or barrier semaphores. Data moves between devices by JAX's collectives and lax.ppermute only.
A program may use at most 128 MiB of HBM per device.

```python
import math
import jax
import jax.numpy as jnp
from jax import lax

D = 2048
HEADS = 16
HEAD_DIM = 128
BLOCK = 64
NEIGHBORS = 2
NEIGH_LEN = 128
BLOCK_DEV = 16
TOKENS = 16384
BLOCKS = 256


def draw_neighbor_bank(key, part):
    key_base = jax.random.fold_in(jax.random.fold_in(key, 11), 0)
    rows = NEIGHBORS * NEIGH_LEN
    base = jnp.clip(jax.random.normal(key_base, (BLOCKS, rows, D), jnp.float32) * 2.0, -8.0, 8.0)
    return base.astype(jnp.bfloat16)


def plant(drawn, own_key, low, largest):
    dims = drawn.shape
    spot = [jax.random.randint(jax.random.fold_in(own_key, axis), (), 0, dims[axis]) for axis in range(len(dims))]
    drawn = drawn.at[tuple(spot)].set(low)
    longest = dims.index(max(dims))
    spot[longest] = (spot[longest] + 1) % dims[longest]
    return drawn.at[tuple(spot)].set(largest)


def block_scale(rng, extent, cuts, smallest, high):
    def one(dim, parts):
        steps = jax.random.uniform(jax.random.fold_in(jax.random.fold_in(rng, 6), dim), (parts,), jnp.float32, smallest / len(cuts), high / len(cuts))
        return jnp.repeat(jnp.exp(steps), extent[dim] // parts).reshape((-1,) + (1,) * (len(extent) - dim - 1))

    loudness = one(*cuts[0])
    for cut in cuts[1:]:
        loudness = loudness * one(*cut)
    return loudness


def noise(key, dims, scale, reach, cuts=(), kind=jnp.bfloat16):
    entries = jax.random.normal(key, dims, jnp.float32) * scale
    if len(cuts) > 0:
        entries = block_scale(key, dims, cuts, -0.22, 0.18) * entries
    return jnp.clip(entries, min=-reach, max=reach).astype(kind)


def setup_inputs(seed: int = 0, part: int = 0) -> dict:
    streams_of = jax.random.split(jax.random.key(seed), 8)
    part_splits = jax.random.split(jax.random.fold_in(streams_of[7], part), 8)
    tokens = noise(part_splits[0], (TOKENS, D), 1.0, 6.0, ((0, 16),))
    neighbor_bank = draw_neighbor_bank(jax.random.fold_in(jax.random.fold_in(streams_of[7], part), 71), part)
    slots = plant(jax.random.randint(part_splits[2], (BLOCKS,), 0, BLOCK_DEV), jax.random.fold_in(part_splits[2], 1), 0, BLOCK_DEV - 1).astype(jnp.int32)
    w_query = noise(streams_of[3], (D, D), D ** -0.5, 0.125, ((0, 16), (1, 4)))
    w_key = noise(streams_of[4], (D, D), D ** -0.5, 0.125, ((0, 16), (1, 4)))
    w_value = noise(streams_of[5], (D, D), D ** -0.5, 0.125, ((0, 16), (1, 4)))
    w_out = noise(streams_of[6], (D, D), D ** -0.5, 0.125, ((0, 4), (1, 16)))
    return {"tokens": tokens, "neighbor_bank": neighbor_bank, "slots": slots, "w_query": w_query, "w_key": w_key, "w_value": w_value, "w_out": w_out}


def rms_normed(tokens):
    hidden = tokens.astype(jnp.float32)
    scale_row = lax.rsqrt(lax.optimization_barrier(jnp.mean(hidden * hidden, axis=-1, keepdims=True)) + 1e-06)
    return (hidden * scale_row).astype(jnp.bfloat16)

def reference(tokens, neighbor_bank, slots, w_query, w_key, w_value, w_out):
    normed = rms_normed(tokens)
    queries = jnp.dot(normed, w_query, preferred_element_type=jnp.float32).astype(jnp.bfloat16)
    block_ids = jnp.arange(BLOCKS, dtype=jnp.int32)
    bank_rows = (block_ids // BLOCK_DEV * BLOCK_DEV + slots).astype(jnp.int32)
    retrieved = jnp.take(neighbor_bank, bank_rows, axis=0).reshape(BLOCKS * NEIGHBORS * NEIGH_LEN, D)
    key_rows = jnp.dot(retrieved, w_key, preferred_element_type=jnp.float32).astype(jnp.bfloat16)
    value_rows = jnp.dot(retrieved, w_value, preferred_element_type=jnp.float32).astype(jnp.bfloat16)
    key_rows = key_rows.reshape(BLOCKS, NEIGHBORS * NEIGH_LEN, HEADS, HEAD_DIM)
    value_rows = value_rows.reshape(BLOCKS, NEIGHBORS * NEIGH_LEN, HEADS, HEAD_DIM)
    padding = jnp.zeros((1, NEIGHBORS * NEIGH_LEN, HEADS, HEAD_DIM), jnp.bfloat16)
    prior_keys = jnp.concatenate([padding, key_rows[:-1]], axis=0)
    prior_values = jnp.concatenate([padding, value_rows[:-1]], axis=0)
    query_blocks = queries.reshape(BLOCKS, BLOCK, HEADS, HEAD_DIM)
    scores = jnp.einsum('cmhd,cnhd->chmn', query_blocks.astype(jnp.float32), prior_keys.astype(jnp.float32)) / math.sqrt(HEAD_DIM)
    peak_score = lax.optimization_barrier(jnp.max(scores, axis=-1, keepdims=True))
    exponent = jnp.exp(scores - peak_score)
    weights = (exponent / lax.optimization_barrier(jnp.sum(exponent, axis=-1, keepdims=True))).astype(jnp.bfloat16)
    attended = jnp.einsum('chmn,cnhd->cmhd', weights.astype(jnp.float32), prior_values.astype(jnp.float32))
    attended = attended.astype(jnp.bfloat16).reshape(TOKENS, D)
    return jnp.dot(attended, w_out, preferred_element_type=jnp.float32).astype(jnp.bfloat16)
```

```python
import functools
import math

import jax
import jax.numpy as jnp
from jax import lax
from jax.experimental import pallas as pl
from jax.experimental.pallas import tpu as pltpu
from jax.sharding import PartitionSpec as P

HEAD_DIM = 128
X_LO, Z, CORE, X = 2, 4, 2, 4
CHUNK_HEADS = (2, 2)
TOKEN_PARTS = 2
GROUP = 2


def route(move):
    pairs = []
    for x in range(X):
        for z in range(Z):
            for c in range(CORE):
                to_x, to_z, to_c = move(x, z, c)
                to_x, to_z, to_c = to_x % X, to_z % Z, to_c % CORE
                src = (((x % X_LO) * Z + z) * CORE + c) * 2 + x // X_LO
                dst = (((to_x % X_LO) * Z + to_z) * CORE + to_c) * 2 + to_x // X_LO
                pairs.append((src, dst))
    return pairs


Z_UP = route(lambda x, z, c: (x, z + 1, c))
Z_DOWN = route(lambda x, z, c: (x, z - 1, c))
Z_FAR = route(lambda x, z, c: (x, z + 2, c))
X_UP = route(lambda x, z, c: (x + 1, z, c))
X_DOWN = route(lambda x, z, c: (x - 1, z, c))
OTHER_CORE = route(lambda x, z, c: (x, z, c + 1))


def plane(block, pairs):
    return lax.ppermute(block, ("seq", "batch"), pairs)


def gather_weights(shard):
    below = plane(shard, Z_UP)
    above = plane(shard, Z_DOWN)
    far = plane(shard, Z_FAR)
    near_pair = jnp.stack([shard, below])
    far_pair = jnp.stack([above, far])
    x_near = plane(near_pair, X_UP)
    x_far = plane(far_pair, X_DOWN)
    mine = [near_pair, far_pair, x_near, x_far]
    return mine + [plane(p, OTHER_CORE) for p in mine]


def origins(me):
    x_lo, z, c = me // (Z * CORE), (me // CORE) % Z, me % CORE
    found = []
    for core in (c, 1 - c):
        for x in (x_lo, 1 - x_lo):
            for dz in (0, 3, 1, 2):
                found.append((x * Z + (z + dz) % Z) * CORE + core)
    return jnp.stack(found).astype(jnp.int32)


def attend_kernel(heads, first, group, slots, rows, bank, arrived, normed, *rest):
    pieces, out, ctx, w, ctx_sem, w_sem = rest[:8], *rest[8:]
    step, steps = pl.program_id(0), pl.num_programs(0)
    width = heads * HEAD_DIM
    kv_rows = bank.shape[1]
    shard = pieces[0].shape[1]

    def fetch(g, slot):
        for j in range(group):
            c = first + g * group + j
            dst = ctx.at[slot, pl.ds(j * kv_rows, kv_rows), :]
            sem = ctx_sem.at[slot]
            if first == 0 and j == 0:

                @pl.when(g == 0)
                def _():
                    pltpu.make_async_copy(arrived, dst, sem).start()

                @pl.when(g > 0)
                def _():
                    pltpu.make_async_copy(bank.at[slots[jnp.maximum(c - 1, 0)]], dst, sem).start()
            else:
                pltpu.make_async_copy(bank.at[slots[c - 1]], dst, sem).start()

    @pl.when(step == 0)
    def _():
        for i in range(8):
            for k in range(2):
                at = pl.multiple_of(rows[i * 2 + k] * shard, shard)
                pltpu.make_async_copy(pieces[i].at[k], w.at[pl.ds(at, shard), :], w_sem).start()
        fetch(0, 0)

    @pl.when(step + 1 < steps)
    def _():
        fetch(step + 1, (step + 1) % 2)

    @pl.when(step == 0)
    def _():
        pltpu.make_async_copy(w, w, w_sem).wait()

    slot = step % 2
    q = jnp.dot(normed[...], w[:, :width], preferred_element_type=jnp.float32).astype(jnp.bfloat16)
    pltpu.make_async_copy(ctx.at[slot], ctx.at[slot], ctx_sem.at[slot]).wait()
    kv = jnp.dot(ctx[slot], w[:, width:], preferred_element_type=jnp.float32).astype(jnp.bfloat16)
    block = normed.shape[0] // group
    for j in range(group):
        for h in range(heads):
            qh = q[j * block : (j + 1) * block, h * HEAD_DIM : (h + 1) * HEAD_DIM]
            kh = kv[j * kv_rows : (j + 1) * kv_rows, h * HEAD_DIM : (h + 1) * HEAD_DIM]
            vh = kv[j * kv_rows : (j + 1) * kv_rows, width + h * HEAD_DIM : width + (h + 1) * HEAD_DIM]
            s = lax.dot_general(qh, kh, (((1,), (1,)), ((), ())), preferred_element_type=jnp.float32)
            s = s * (1.0 / math.sqrt(HEAD_DIM))
            e = jnp.exp(s - jnp.max(s, axis=-1, keepdims=True))
            p = (e / jnp.sum(e, axis=-1, keepdims=True)).astype(jnp.bfloat16)
            o = jnp.dot(p, vh, preferred_element_type=jnp.float32)
            out[j * block : (j + 1) * block, h * HEAD_DIM : (h + 1) * HEAD_DIM] = o.astype(jnp.bfloat16)


def attend(slots, rows, bank, arrived, normed, pieces, heads, first, blocks, group):
    model = normed.shape[1]
    kv_rows = bank.shape[1]
    block = normed.shape[0] // bank.shape[0]
    width = heads * HEAD_DIM
    hbm = pl.BlockSpec(memory_space=pl.ANY)
    flops = 2 * blocks * (2 * kv_rows + block) * model * width
    return pl.pallas_call(
        functools.partial(attend_kernel, heads, first, group),
        out_shape=jax.ShapeDtypeStruct((blocks * block, width), jnp.bfloat16),
        grid_spec=pltpu.PrefetchScalarGridSpec(
            num_scalar_prefetch=2,
            grid=(blocks // group,),
            in_specs=[hbm, hbm, pl.BlockSpec((group * block, model), lambda i, *_: (first // group + i, 0))]
            + [hbm] * 8,
            out_specs=pl.BlockSpec((group * block, width), lambda i, *_: (i, 0)),
            scratch_shapes=[
                pltpu.VMEM((2, group * kv_rows, model), jnp.bfloat16),
                pltpu.VMEM((model, 3 * width), jnp.bfloat16),
                pltpu.SemaphoreType.DMA((2,)),
                pltpu.SemaphoreType.DMA,
            ],
        ),
        cost_estimate=pl.CostEstimate(
            flops=flops, bytes_accessed=2 * blocks * kv_rows * model, transcendentals=0
        ),
        name="attend",
    )(slots, rows, bank, arrived, normed, *pieces)


def project_kernel(chunks, rows, cols, *refs):
    n = 4 * chunks
    parts, pieces = refs[:n], refs[n : n + 8]
    out, att, w, att_sem, w_sem = refs[-5:]
    deep, wide = pieces[0].shape[1:]
    for i in range(8):
        for k in range(2):
            origin = rows[i * 2 + k]
            r = pl.multiple_of((origin // 4) * deep, deep)
            c = pl.multiple_of((origin % 4) * wide, wide)
            pltpu.make_async_copy(pieces[i].at[k], w.at[pl.ds(r, deep), pl.ds(c, wide)], w_sem).start()
    at = 0
    for i in range(chunks):
        width = parts[4 * i].shape[1]
        for k in range(4):
            c = pl.multiple_of(cols[k] * deep + at, HEAD_DIM)
            pltpu.make_async_copy(parts[4 * i + k], att.at[:, pl.ds(c, width)], att_sem).start()
        at += width
    pltpu.make_async_copy(w, w, w_sem).wait()
    pltpu.make_async_copy(att, att, att_sem).wait()
    out[...] = jnp.dot(att[...], w[...], preferred_element_type=jnp.float32).astype(jnp.bfloat16)


def project(rows, cols, parts, pieces, token_part, out_rows, before):
    tall = parts[0].shape[0]
    model = 4 * pieces[0].shape[1]
    wide = 4 * pieces[0].shape[2]
    hbm = pl.BlockSpec(memory_space=pl.ANY)
    extra = [] if before is None else [before]
    return pl.pallas_call(
        functools.partial(project_kernel, len(parts) // 4),
        out_shape=jax.ShapeDtypeStruct((out_rows, wide), jnp.bfloat16),
        grid_spec=pltpu.PrefetchScalarGridSpec(
            num_scalar_prefetch=2,
            grid=(1,),
            in_specs=[hbm] * (len(parts) + 8 + len(extra)),
            out_specs=pl.BlockSpec((tall, wide), lambda i, *_: (token_part, 0)),
            scratch_shapes=[
                pltpu.VMEM((tall, model), jnp.bfloat16),
                pltpu.VMEM((model, wide), jnp.bfloat16),
                pltpu.SemaphoreType.DMA,
                pltpu.SemaphoreType.DMA,
            ],
        ),
        input_output_aliases={} if before is None else {2 + len(parts) + 8: 0},
        cost_estimate=pl.CostEstimate(
            flops=2 * tall * model * wide, bytes_accessed=2 * model * (tall + wide), transcendentals=0
        ),
        name="project",
    )(rows, cols, *parts, *pieces, *extra)


def local(tokens, neighbor_bank, slots, w_query, w_key, w_value, w_out):
    blocks = neighbor_bank.shape[0]
    me, head_at = lax.axis_index("seq"), lax.axis_index("head")
    rows = origins(me)
    cols = jnp.stack([(head_at + d) % 4 for d in (0, 3, 1, 2)]).astype(jnp.int32)

    chunk_pieces = []
    at = 0
    for heads in CHUNK_HEADS:
        span = slice(at * HEAD_DIM, (at + heads) * HEAD_DIM)
        shard = jnp.concatenate([w[:, span] for w in (w_query, w_key, w_value)], axis=1)
        chunk_pieces.append(gather_weights(shard))
        at += heads
    swap = [
        ((4 * a + j) * 4 + b, (4 * b + j) * 4 + a) for a in range(4) for b in range(4) for j in range(4)
    ]
    out_pieces = gather_weights(lax.ppermute(w_out, ("seq", "head"), swap))

    last = lax.dynamic_index_in_dim(neighbor_bank, slots[blocks - 1], 0, keepdims=False)
    devices = lax.axis_size("seq")
    arrived = lax.ppermute(last, "seq", [(i, i + 1) for i in range(devices - 1)])

    hidden = tokens.astype(jnp.float32)
    normed = (hidden * lax.rsqrt(jnp.mean(hidden * hidden, axis=-1, keepdims=True) + 1e-06)).astype(
        jnp.bfloat16
    )

    part_blocks = blocks // TOKEN_PARTS
    parts = [[] for _ in range(TOKEN_PARTS)]
    ring = lambda block, d: lax.ppermute(block, "head", [(i, (i + d) % 4) for i in range(4)])
    for heads, pieces in zip(CHUNK_HEADS, chunk_pieces):
        for t in range(TOKEN_PARTS):
            own = attend(
                slots, rows, neighbor_bank, arrived, normed, pieces, heads, t * part_blocks, part_blocks, GROUP
            )
            parts[t] += [own, ring(own, 1), ring(own, -1), ring(own, 2)]
    out = None
    for t in range(TOKEN_PARTS):
        out = project(rows, cols, parts[t], out_pieces, t, tokens.shape[0], out)
    return out


def solution(mesh):
    in_specs = (
        P(("batch", "seq"), None),
        P(("batch", "seq"), None, None),
        P(("batch", "seq")),
        P("seq", "head"),
        P("seq", "head"),
        P("seq", "head"),
        P("head", "seq"),
    )
    out_specs = P(("batch", "seq"), "head")
    return jax.shard_map(local, mesh=mesh, in_specs=in_specs, out_specs=out_specs, check_vma=False)
```

```python
import functools
import math

import jax
import jax.numpy as jnp
from jax import lax
from jax.experimental import pallas as pl
from jax.experimental.pallas import tpu as pltpu
from jax.sharding import PartitionSpec as P

HEAD_DIM = 128
X_LO, Z, CORE, X = 2, 4, 2, 4
CHUNK_HEADS = (2, 2)
TOKEN_PARTS = 2
GROUP = 4
LAG = 1


def route(move):
    pairs = []
    for x in range(X):
        for z in range(Z):
            for c in range(CORE):
                to_x, to_z, to_c = move(x, z, c)
                to_x, to_z, to_c = to_x % X, to_z % Z, to_c % CORE
                src = (((x % X_LO) * Z + z) * CORE + c) * 2 + x // X_LO
                dst = (((to_x % X_LO) * Z + to_z) * CORE + to_c) * 2 + to_x // X_LO
                pairs.append((src, dst))
    return pairs


Z_UP = route(lambda x, z, c: (x, z + 1, c))
Z_DOWN = route(lambda x, z, c: (x, z - 1, c))
Z_FAR = route(lambda x, z, c: (x, z + 2, c))
X_UP = route(lambda x, z, c: (x + 1, z, c))
X_DOWN = route(lambda x, z, c: (x - 1, z, c))
OTHER_CORE = route(lambda x, z, c: (x, z, c + 1))


def plane(block, pairs):
    return lax.ppermute(block, ("seq", "batch"), pairs)


def after(value, *earlier):
    return lax.optimization_barrier((value, *earlier))[0]


def gather_z(shard):
    return [shard, plane(shard, Z_UP), plane(shard, Z_DOWN), plane(shard, Z_FAR)]


def gather_x(around):
    near_pair, far_pair = jnp.stack(around[:2]), jnp.stack(around[2:])
    return [near_pair, far_pair, plane(near_pair, X_UP), plane(far_pair, X_DOWN)]


def gather_core(mine):
    return mine + [plane(p, OTHER_CORE) for p in mine]


def pack_kernel(at, heads, *refs):
    ins, (out, sem) = refs[:-2], refs[-2:]
    for i in range(3):
        for h in range(heads):
            cols = pl.ds((at + h) * HEAD_DIM, HEAD_DIM)
            pltpu.make_async_copy(ins[i].at[:, cols], out.at[i * heads + h], sem).start()
    if len(ins) > 3:
        for i in range(out.shape[0] - 3 * heads):
            rows = pl.ds(i * HEAD_DIM, HEAD_DIM)
            pltpu.make_async_copy(ins[3].at[rows], out.at[3 * heads + i], sem).start()
    pltpu.make_async_copy(out, out, sem).wait()


def pack(weights, at, heads, *tail):
    count = 3 * heads + sum(t.shape[0] // HEAD_DIM for t in tail)
    return pl.pallas_call(
        functools.partial(pack_kernel, at, heads),
        out_shape=jax.ShapeDtypeStruct((count, weights[0].shape[0], HEAD_DIM), jnp.bfloat16),
        in_specs=[pl.BlockSpec(memory_space=pl.ANY)] * (3 + len(tail)),
        out_specs=pl.BlockSpec(memory_space=pltpu.VMEM),
        scratch_shapes=[pltpu.SemaphoreType.DMA],
        name="pack",
    )(*weights, *tail)


def origins(me):
    x_lo, z, c = me // (Z * CORE), (me // CORE) % Z, me % CORE
    found = []
    for core in (c, 1 - c):
        for x in (x_lo, 1 - x_lo):
            for dz in (0, 3, 1, 2):
                found.append((x * Z + (z + dz) % Z) * CORE + core)
    return jnp.stack(found).astype(jnp.int32)


def only_head(q, h, heads):
    empty = jnp.zeros((q.shape[0], HEAD_DIM), q.dtype)
    return jnp.concatenate(
        [q[:, i * HEAD_DIM : (i + 1) * HEAD_DIM] if i == h else empty for i in range(heads)], axis=1
    )


def attend_kernel(heads, first, group, slots, rows, bank, normed, *rest):
    arrived, rest = (rest[0], rest[1:]) if first == 0 else (None, rest)
    pieces, out, ctx, w, ctx_sem, w_sem = rest[:8], *rest[8:]
    step, steps = pl.program_id(0), pl.num_programs(0)
    width = heads * HEAD_DIM
    kv_rows = bank.shape[1]
    shard = pieces[0].shape[2]

    def fetch(g, slot):
        for j in range(group):
            c = first + g * group + j
            dst = ctx.at[slot, pl.ds(j * kv_rows, kv_rows), :]
            sem = ctx_sem.at[slot]
            if first == 0 and j == 0:

                @pl.when(g == 0)
                def _():
                    pltpu.make_async_copy(arrived, dst, sem).start()

                @pl.when(g > 0)
                def _():
                    pltpu.make_async_copy(bank.at[slots[jnp.maximum(c - 1, 0)]], dst, sem).start()
            else:
                pltpu.make_async_copy(bank.at[slots[c - 1]], dst, sem).start()

    @pl.when(step == 0)
    def _():
        for i in range(8):
            for k in range(2):
                at = pl.multiple_of(rows[i * 2 + k] * shard, shard)
                pltpu.make_async_copy(
                    pieces[i].at[k, pl.ds(0, 3 * heads)], w.at[:, pl.ds(at, shard), :], w_sem
                ).start()
        fetch(0, 0)

    @pl.when(step + 1 < steps)
    def _():
        fetch(step + 1, (step + 1) % 2)

    @pl.when(step == 0)
    def _():
        pltpu.make_async_copy(w, w, w_sem).wait()

    slot = step % 2
    wq = jnp.concatenate([w[i] for i in range(heads)], axis=1)
    wkv = jnp.concatenate([w[i] for i in range(heads, 3 * heads)], axis=1)
    q = jnp.dot(normed[...], wq, preferred_element_type=jnp.float32).astype(jnp.bfloat16)
    pltpu.make_async_copy(ctx.at[slot], ctx.at[slot], ctx_sem.at[slot]).wait()
    block = normed.shape[0] // group
    kv, weights = {}, {}
    for j in range(group + 2 * LAG):
        if j < group:
            kv[j] = jnp.dot(
                ctx[slot, j * kv_rows : (j + 1) * kv_rows], wkv, preferred_element_type=jnp.float32
            ).astype(jnp.bfloat16)
        i = j - LAG
        if 0 <= i < group:
            qi = q[i * block : (i + 1) * block]
            stacked = jnp.concatenate([only_head(qi, h, heads) for h in range(heads)], axis=0)
            s = lax.dot_general(
                stacked, kv[i][:, :width], (((1,), (1,)), ((), ())), preferred_element_type=jnp.float32
            )
            s = s * (1.0 / math.sqrt(HEAD_DIM))
            e = jnp.exp(s - jnp.max(s, axis=-1, keepdims=True))
            weights[i] = (e / jnp.sum(e, axis=-1, keepdims=True)).astype(jnp.bfloat16)
        i = j - 2 * LAG
        if 0 <= i < group:
            o = jnp.dot(weights[i], kv[i][:, width:], preferred_element_type=jnp.float32).astype(jnp.bfloat16)
            for h in range(heads):
                cols = slice(h * HEAD_DIM, (h + 1) * HEAD_DIM)
                out[i * block : (i + 1) * block, cols] = o[h * block : (h + 1) * block, cols]


def attend(slots, rows, bank, arrived, normed, pieces, heads, first, blocks, group):
    model = normed.shape[1]
    kv_rows = bank.shape[1]
    arrived = [arrived] if first == 0 else []
    block = normed.shape[0] // bank.shape[0]
    width = heads * HEAD_DIM
    hbm = pl.BlockSpec(memory_space=pl.ANY)
    flops = 2 * blocks * (2 * kv_rows + block) * model * width
    return pl.pallas_call(
        functools.partial(attend_kernel, heads, first, group),
        out_shape=jax.ShapeDtypeStruct((blocks * block, width), jnp.bfloat16),
        grid_spec=pltpu.PrefetchScalarGridSpec(
            num_scalar_prefetch=2,
            grid=(blocks // group,),
            in_specs=[hbm, pl.BlockSpec((group * block, model), lambda i, *_: (first // group + i, 0))]
            + [hbm] * (len(arrived) + 8),
            out_specs=pl.BlockSpec((group * block, width), lambda i, *_: (i, 0)),
            scratch_shapes=[
                pltpu.VMEM((2, group * kv_rows, model), jnp.bfloat16),
                pltpu.VMEM((3 * heads, model, HEAD_DIM), jnp.bfloat16),
                pltpu.SemaphoreType.DMA((2,)),
                pltpu.SemaphoreType.DMA,
            ],
        ),
        cost_estimate=pl.CostEstimate(
            flops=flops, bytes_accessed=2 * blocks * kv_rows * model, transcendentals=0
        ),
        compiler_params=pltpu.CompilerParams(vmem_limit_bytes=32 * 2**20),
        name="attend",
    )(slots, rows, bank, normed, *arrived, *pieces)


def project_kernel(chunks, rows, cols, *refs):
    n = 4 * chunks
    parts, pieces = refs[:n], refs[n : n + 8]
    out, att, w, att_sem, w_sem = refs[-5:]
    deep, wide = att.shape[1] // 4, w.shape[1] // 4
    tile = pieces[0].shape[2]
    lead = pieces[0].shape[1] - deep // tile
    for i in range(8):
        for k in range(2):
            origin = rows[i * 2 + k]
            r = pl.multiple_of((origin // 4) * deep, deep)
            c = pl.multiple_of((origin % 4) * wide, wide)
            for t in range(deep // tile):
                pltpu.make_async_copy(
                    pieces[i].at[k, lead + t], w.at[pl.ds(r + t * tile, tile), pl.ds(c, wide)], w_sem
                ).start()
    at = 0
    for i in range(chunks):
        width = parts[4 * i].shape[1]
        for k in range(4):
            c = pl.multiple_of(cols[k] * deep + at, HEAD_DIM)
            pltpu.make_async_copy(parts[4 * i + k], att.at[:, pl.ds(c, width)], att_sem).start()
        at += width
    pltpu.make_async_copy(w, w, w_sem).wait()
    pltpu.make_async_copy(att, att, att_sem).wait()
    out[...] = jnp.dot(att[...], w[...], preferred_element_type=jnp.float32).astype(jnp.bfloat16)


def project(rows, cols, parts, pieces, token_part, out_rows, model, wide, before):
    tall = parts[0].shape[0]
    hbm = pl.BlockSpec(memory_space=pl.ANY)
    extra = [] if before is None else [before]
    return pl.pallas_call(
        functools.partial(project_kernel, len(parts) // 4),
        out_shape=jax.ShapeDtypeStruct((out_rows, wide), jnp.bfloat16),
        grid_spec=pltpu.PrefetchScalarGridSpec(
            num_scalar_prefetch=2,
            grid=(1,),
            in_specs=[hbm] * (len(parts) + 8 + len(extra)),
            out_specs=pl.BlockSpec((tall, wide), lambda i, *_: (token_part, 0)),
            scratch_shapes=[
                pltpu.VMEM((tall, model), jnp.bfloat16),
                pltpu.VMEM((model, wide), jnp.bfloat16),
                pltpu.SemaphoreType.DMA,
                pltpu.SemaphoreType.DMA,
            ],
        ),
        input_output_aliases={} if before is None else {2 + len(parts) + 8: 0},
        cost_estimate=pl.CostEstimate(
            flops=2 * tall * model * wide, bytes_accessed=2 * model * (tall + wide), transcendentals=0
        ),
        compiler_params=pltpu.CompilerParams(vmem_limit_bytes=16 * 2**20),
        name="project",
    )(rows, cols, *parts, *pieces, *extra)


def local(tokens, neighbor_bank, slots, w_query, w_key, w_value, w_out):
    blocks = neighbor_bank.shape[0]
    me, head_at = lax.axis_index("seq"), lax.axis_index("head")
    rows = origins(me)
    cols = jnp.stack([(head_at + d) % 4 for d in (0, 3, 1, 2)]).astype(jnp.int32)

    swap = [
        ((4 * a + j) * 4 + b, (4 * b + j) * 4 + a) for a in range(4) for b in range(4) for j in range(4)
    ]
    weights = (w_query, w_key, w_value)
    z_first = gather_z(pack(weights, 0, CHUNK_HEADS[0]))
    out_shard = lax.ppermute(w_out, ("seq", "head"), swap)
    hidden = tokens.astype(jnp.float32)
    normed = (hidden * lax.rsqrt(jnp.mean(hidden * hidden, axis=-1, keepdims=True) + 1e-06)).astype(
        jnp.bfloat16
    )
    last = lax.dynamic_index_in_dim(neighbor_bank, slots[blocks - 1], 0, keepdims=False)

    x_first = gather_x(z_first)
    second = pack(weights, CHUNK_HEADS[0], CHUNK_HEADS[1], out_shard)
    z_second = gather_z(after(second, *z_first))
    devices = lax.axis_size("seq")
    arrived = lax.ppermute(after(last, *z_first), "seq", [(i, i + 1) for i in range(devices - 1)])
    pieces = gather_core(x_first)

    part_blocks = blocks // TOKEN_PARTS
    parts = [[] for _ in range(TOKEN_PARTS)]
    ring = lambda block, d: lax.ppermute(block, "head", [(i, (i + d) % 4) for i in range(4)])
    own, n = None, 0
    for heads in CHUNK_HEADS:
        for t in reversed(range(TOKEN_PARTS)):
            x = normed if own is None else after(normed, own)
            own = attend(
                slots, rows, neighbor_bank, arrived, x, pieces, heads, t * part_blocks, part_blocks, GROUP
            )
            parts[t] += [own, ring(own, 1), ring(own, -1), ring(own, 2)]
            if n == 0:
                x_second = gather_x([after(p, own) for p in z_second])
            if n == 1:
                pieces = gather_core(x_second)
            n += 1
    out = None
    for t in reversed(range(TOKEN_PARTS)):
        out = project(
            rows, cols, parts[t], pieces, t, tokens.shape[0], tokens.shape[1], w_out.shape[0], out
        )
    return out


def solution(mesh):
    in_specs = (
        P(("batch", "seq"), None),
        P(("batch", "seq"), None, None),
        P(("batch", "seq")),
        P("seq", "head"),
        P("seq", "head"),
        P("seq", "head"),
        P("head", "seq"),
    )
    out_specs = P(("batch", "seq"), "head")

    return jax.shard_map(local, mesh=mesh, in_specs=in_specs, out_specs=out_specs, check_vma=False)
```

```python
import functools
import math

import jax
import jax.numpy as jnp
from jax import lax
from jax.experimental import pallas as pl
from jax.experimental.pallas import tpu as pltpu
from jax.sharding import PartitionSpec as P

HEAD_DIM = 128
X_LO, Z, CORE, X = 2, 4, 2, 4
CHUNK_HEADS = (2, 2)
RUNS = ((12, 4), (0, 12))
GROUP = 4
LAG = 1
AHEAD = 1


def route(move):
    pairs = []
    for x in range(X):
        for z in range(Z):
            for c in range(CORE):
                to_x, to_z, to_c = move(x, z, c)
                to_x, to_z, to_c = to_x % X, to_z % Z, to_c % CORE
                src = (((x % X_LO) * Z + z) * CORE + c) * 2 + x // X_LO
                dst = (((to_x % X_LO) * Z + to_z) * CORE + to_c) * 2 + to_x // X_LO
                pairs.append((src, dst))
    return pairs


Z_UP = route(lambda x, z, c: (x, z + 1, c))
Z_DOWN = route(lambda x, z, c: (x, z - 1, c))
Z_FAR = route(lambda x, z, c: (x, z + 2, c))
X_UP = route(lambda x, z, c: (x + 1, z, c))
X_DOWN = route(lambda x, z, c: (x - 1, z, c))
OTHER_CORE = route(lambda x, z, c: (x, z, c + 1))


def plane(block, pairs):
    return lax.ppermute(block, ("seq", "batch"), pairs)


def after(value, *earlier):
    return lax.optimization_barrier((value, *earlier))[0]


def gather_z(shard):
    return [shard, plane(shard, Z_UP), plane(shard, Z_DOWN), plane(shard, Z_FAR)]


def gather_x(around):
    near_pair, far_pair = jnp.stack(around[:2]), jnp.stack(around[2:])
    return [near_pair, far_pair, plane(near_pair, X_UP), plane(far_pair, X_DOWN)]


def gather_core(mine):
    near = [plane(p, OTHER_CORE) for p in mine[:2]]
    far = [plane(p, OTHER_CORE) for p in mine[2:]]
    return mine + near + far


def prepare_kernel(slots, bank, tokens, normed, last, sem):
    step = pl.program_id(0)

    @pl.when(step == 0)
    def _():
        pltpu.make_async_copy(bank.at[slots[bank.shape[0] - 1]], last, sem).start()

    hidden = tokens[...].astype(jnp.float32)
    scale = lax.rsqrt(jnp.mean(hidden * hidden, axis=-1, keepdims=True) + 1e-06)
    normed[...] = (hidden * scale).astype(jnp.bfloat16)

    @pl.when(step == pl.num_programs(0) - 1)
    def _():
        pltpu.make_async_copy(last, last, sem).wait()


def prepare(slots, bank, tokens):
    rows = pl.BlockSpec((tokens.shape[0] // 2, tokens.shape[1]), lambda i, *_: (i, 0))
    return pl.pallas_call(
        prepare_kernel,
        out_shape=(
            jax.ShapeDtypeStruct(tokens.shape, jnp.bfloat16),
            jax.ShapeDtypeStruct(bank.shape[1:], jnp.bfloat16),
        ),
        grid_spec=pltpu.PrefetchScalarGridSpec(
            num_scalar_prefetch=1,
            grid=(2,),
            in_specs=[pl.BlockSpec(memory_space=pl.ANY), rows],
            out_specs=[rows, pl.BlockSpec(bank.shape[1:], lambda i, *_: (0, 0))],
            scratch_shapes=[pltpu.SemaphoreType.DMA],
        ),
        cost_estimate=pl.CostEstimate(flops=2**30, bytes_accessed=2**23, transcendentals=0),
        name="prepare",
    )(slots, bank, tokens)


def pack_kernel(at, heads, *refs):
    ins, (out, sem) = refs[:-2], refs[-2:]
    for i in range(3):
        for h in range(heads):
            cols = pl.ds((at + h) * HEAD_DIM, HEAD_DIM)
            pltpu.make_async_copy(ins[i].at[:, cols], out.at[i * heads + h], sem).start()
    if len(ins) > 3:
        for i in range(out.shape[0] - 3 * heads):
            rows = pl.ds(i * HEAD_DIM, HEAD_DIM)
            pltpu.make_async_copy(ins[3].at[rows], out.at[3 * heads + i], sem).start()
    pltpu.make_async_copy(out, out, sem).wait()


def pack(weights, at, heads, *tail):
    count = 3 * heads + sum(t.shape[0] // HEAD_DIM for t in tail)
    return pl.pallas_call(
        functools.partial(pack_kernel, at, heads),
        out_shape=jax.ShapeDtypeStruct((count, weights[0].shape[0], HEAD_DIM), jnp.bfloat16),
        in_specs=[pl.BlockSpec(memory_space=pl.ANY)] * (3 + len(tail)),
        out_specs=pl.BlockSpec(memory_space=pltpu.VMEM),
        scratch_shapes=[pltpu.SemaphoreType.DMA],
        name="pack",
    )(*weights, *tail)


def origins(me):
    x_lo, z, c = me // (Z * CORE), (me // CORE) % Z, me % CORE
    found = []
    for core in (c, 1 - c):
        for x in (x_lo, 1 - x_lo):
            for dz in (0, 3, 1, 2):
                found.append((x * Z + (z + dz) % Z) * CORE + core)
    return jnp.stack(found).astype(jnp.int32)


def only_head(q, h, heads):
    empty = jnp.zeros((q.shape[0], HEAD_DIM), q.dtype)
    return jnp.concatenate(
        [q[:, i * HEAD_DIM : (i + 1) * HEAD_DIM] if i == h else empty for i in range(heads)], axis=1
    )


def attend_kernel(heads, first, group, skip, slots, rows, bank, normed, *rest):
    arrived, rest = (rest[0], rest[1:]) if first == 0 else (None, rest)
    pieces, out, ctx, w, x, ctx_sem, w_sem, x_sem = rest[:8], *rest[8 + skip :]
    step, steps = pl.program_id(0), pl.num_programs(0)
    width = heads * HEAD_DIM
    kv_rows = bank.shape[1]
    shard = pieces[0].shape[2]
    block = normed.shape[0] // bank.shape[0]
    tall = group * block

    def fetch_tokens(g, slot):
        at = pl.multiple_of(first * block + g * tall, tall)
        pltpu.make_async_copy(normed.at[pl.ds(at, tall)], x.at[slot], x_sem.at[slot]).start()

    def fetch(g, slot, j):
        c = first + g * group + j
        dst = ctx.at[slot, pl.ds(j * kv_rows, kv_rows), :]
        sem = ctx_sem.at[slot, j]
        if first == 0 and j == 0:

            @pl.when(g == 0)
            def _():
                pltpu.make_async_copy(arrived, dst, sem).start()

            @pl.when(g > 0)
            def _():
                pltpu.make_async_copy(bank.at[slots[jnp.maximum(c - 1, 0)]], dst, sem).start()
        else:
            pltpu.make_async_copy(bank.at[slots[c - 1]], dst, sem).start()

    def fetch_next():
        @pl.when(step + 1 < steps)
        def _():
            fetch_tokens(step + 1, (step + 1) % 2)
            for j in range(group):
                fetch(step + 1, (step + 1) % 2, j)

    @pl.when(step == 0)
    def _():
        for i in range(8):
            for k in range(2):
                at = pl.multiple_of(rows[i * 2 + k] * shard, shard)
                pltpu.make_async_copy(
                    pieces[i].at[k, pl.ds(0, 3 * heads)], w.at[:, pl.ds(at, shard), :], w_sem
                ).start()
        fetch_tokens(0, 0)
        fetch(0, 0, 0)

    slot = step % 2

    def compute(starting):
        if starting:
            pltpu.make_async_copy(w, w, w_sem).wait()
            for j in range(1, group):
                fetch(0, 0, j)
        else:
            fetch_next()
        pltpu.make_async_copy(x.at[slot], x.at[slot], x_sem.at[slot]).wait()
        blocks = [ctx.at[slot, pl.ds(j * kv_rows, kv_rows)] for j in range(group)]
        if not starting:
            for j in range(group):
                pltpu.make_async_copy(blocks[j], blocks[j], ctx_sem.at[slot, j]).wait()
        wq = jnp.concatenate([w[i] for i in range(heads)], axis=1)
        wkv = jnp.concatenate([w[i] for i in range(heads, 3 * heads)], axis=1)
        q = jnp.dot(x[slot], wq, preferred_element_type=jnp.float32).astype(jnp.bfloat16)
        kv, weights = {}, {}
        for j in range(group + 2 * LAG):
            if j < group:
                if starting:
                    pltpu.make_async_copy(blocks[j], blocks[j], ctx_sem.at[slot, j]).wait()
                    if j == AHEAD:
                        fetch_next()
                kv[j] = jnp.dot(blocks[j][...], wkv, preferred_element_type=jnp.float32).astype(jnp.bfloat16)
            i = j - LAG
            if 0 <= i < group:
                qi = q[i * block : (i + 1) * block]
                stacked = jnp.concatenate([only_head(qi, h, heads) for h in range(heads)], axis=0)
                s = lax.dot_general(
                    stacked, kv[i][:, :width], (((1,), (1,)), ((), ())), preferred_element_type=jnp.float32
                )
                s = s * (1.0 / math.sqrt(HEAD_DIM))
                e = jnp.exp(s - jnp.max(s, axis=-1, keepdims=True))
                weights[i] = (e / jnp.sum(e, axis=-1, keepdims=True)).astype(jnp.bfloat16)
            i = j - 2 * LAG
            if 0 <= i < group:
                o = jnp.dot(weights[i], kv[i][:, width:], preferred_element_type=jnp.float32).astype(jnp.bfloat16)
                for h in range(heads):
                    cols = slice(h * HEAD_DIM, (h + 1) * HEAD_DIM)
                    out[i * block : (i + 1) * block, cols] = o[h * block : (h + 1) * block, cols]

    @pl.when(step == 0)
    def _():
        compute(True)

    @pl.when(step > 0)
    def _():
        compute(False)


def attend(slots, rows, bank, arrived, normed, pieces, heads, first, blocks, group, whole=False, into=None):
    model = normed.shape[1]
    kv_rows = bank.shape[1]
    arrived = [arrived] if first == 0 else []
    into = [] if into is None else [into]
    at = first // group if whole else 0
    block = normed.shape[0] // bank.shape[0]
    width = heads * HEAD_DIM
    hbm = pl.BlockSpec(memory_space=pltpu.HBM)
    flops = 2 * blocks * (2 * kv_rows + block) * model * width
    return pl.pallas_call(
        functools.partial(attend_kernel, heads, first, group, len(into)),
        out_shape=jax.ShapeDtypeStruct((normed.shape[0] if whole else blocks * block, width), jnp.bfloat16),
        grid_spec=pltpu.PrefetchScalarGridSpec(
            num_scalar_prefetch=2,
            grid=(blocks // group,),
            in_specs=[hbm] * (2 + len(arrived) + 8 + len(into)),
            out_specs=pl.BlockSpec((group * block, width), lambda i, *_: (at + i, 0)),
            scratch_shapes=[
                pltpu.VMEM((2, group * kv_rows, model), jnp.bfloat16),
                pltpu.VMEM((3 * heads, model, HEAD_DIM), jnp.bfloat16),
                pltpu.VMEM((2, group * block, model), jnp.bfloat16),
                pltpu.SemaphoreType.DMA((2, group)),
                pltpu.SemaphoreType.DMA,
                pltpu.SemaphoreType.DMA((2,)),
            ],
        ),
        input_output_aliases={4 + len(arrived) + 8: 0} if into else {},
        cost_estimate=pl.CostEstimate(
            flops=flops, bytes_accessed=2 * blocks * kv_rows * model, transcendentals=0
        ),
        compiler_params=pltpu.CompilerParams(vmem_limit_bytes=60 * 2**20),
        name="attend",
    )(slots, rows, bank, normed, *arrived, *pieces, *into)


def load_parts(parts, cols, att, start, sem):
    tall, width = parts[0].shape
    for k in range(4):
        c = pl.multiple_of(cols[k] * width, width)
        pltpu.make_async_copy(parts[k], att.at[pl.ds(start, tall), pl.ds(c, width)], sem).start()


def project_first_kernel(rows, cols, *refs):
    parts, pieces = refs[:4], refs[4:12]
    out, w_next, w, att, att_sem, w_sem, next_sem = refs[12:]
    deep, wide = w.shape[0] // 4, w.shape[1] // 4
    tile = pieces[0].shape[2]
    count = deep // tile
    lead = pieces[0].shape[1] - 2 * count
    load_parts(parts, cols, att, 0, att_sem)
    for dst, sem, at in ((w, w_sem, lead), (w_next, next_sem, lead + count)):
        for i in range(8):
            for k in range(2):
                origin = rows[i * 2 + k]
                r = pl.multiple_of((origin // 4) * deep, deep)
                c = pl.multiple_of((origin % 4) * wide, wide)
                for t in range(count):
                    pltpu.make_async_copy(
                        pieces[i].at[k, at + t], dst.at[pl.ds(r + t * tile, tile), pl.ds(c, wide)], sem
                    ).start()
    pltpu.make_async_copy(att, att, att_sem).wait()
    pltpu.make_async_copy(w, w, w_sem).wait()
    out[...] = jnp.dot(att[...], w[...], preferred_element_type=jnp.float32)
    pltpu.make_async_copy(w_next, w_next, next_sem).wait()


def project_first(rows, cols, parts, pieces, wide):
    tall, deep = parts[0].shape[0], 4 * parts[0].shape[1]
    hbm = pl.BlockSpec(memory_space=pltpu.HBM)
    return pl.pallas_call(
        project_first_kernel,
        out_shape=(jax.ShapeDtypeStruct((tall, wide), jnp.float32), jax.ShapeDtypeStruct((deep, wide), jnp.bfloat16)),
        grid_spec=pltpu.PrefetchScalarGridSpec(
            num_scalar_prefetch=2,
            grid=(1,),
            in_specs=[hbm] * 12,
            out_specs=(
                pl.BlockSpec((tall, wide), lambda i, *_: (0, 0)),
                pl.BlockSpec((deep, wide), lambda i, *_: (0, 0)),
            ),
            scratch_shapes=[
                pltpu.VMEM((deep, wide), jnp.bfloat16),
                pltpu.VMEM((tall, deep), jnp.bfloat16),
                pltpu.SemaphoreType.DMA,
                pltpu.SemaphoreType.DMA,
                pltpu.SemaphoreType.DMA,
            ],
        ),
        compiler_params=pltpu.CompilerParams(vmem_limit_bytes=60 * 2**20),
        cost_estimate=pl.CostEstimate(flops=2 * tall * deep * wide, bytes_accessed=2**23, transcendentals=0),
        name="project_first",
    )(rows, cols, *parts, *pieces)


def project_last_kernel(starts, cols, *refs):
    n = 4 * len(starts)
    parts, (w_in, share_in, out, w, share, att, w_sem, sem, att_sem) = refs[:n], refs[n:]
    pltpu.make_async_copy(w_in, w, w_sem).start()
    for i, start in enumerate(starts):
        load_parts(parts[4 * i : 4 * i + 4], cols, att, start, att_sem)
    pltpu.make_async_copy(share_in, share, sem).start()
    pltpu.make_async_copy(w, w, w_sem).wait()
    pltpu.make_async_copy(att, att, att_sem).wait()
    pltpu.make_async_copy(share, share, sem).wait()
    rest = jnp.dot(att[...], w[...], preferred_element_type=jnp.float32)
    out[...] = (share[...] + rest).astype(jnp.bfloat16)


def project_last(cols, runs, weights, share):
    (tall, wide), deep = share.shape, weights.shape[0]
    hbm = pl.BlockSpec(memory_space=pltpu.HBM)
    starts = tuple(start for start, _ in runs)
    parts = [p for _, four in runs for p in four]
    return pl.pallas_call(
        functools.partial(project_last_kernel, starts),
        out_shape=jax.ShapeDtypeStruct((tall, wide), jnp.bfloat16),
        grid_spec=pltpu.PrefetchScalarGridSpec(
            num_scalar_prefetch=1,
            grid=(1,),
            in_specs=[hbm] * (len(parts) + 2),
            out_specs=pl.BlockSpec((tall, wide), lambda i, *_: (0, 0)),
            scratch_shapes=[
                pltpu.VMEM((deep, wide), jnp.bfloat16),
                pltpu.VMEM((tall, wide), jnp.float32),
                pltpu.VMEM((tall, deep), jnp.bfloat16),
                pltpu.SemaphoreType.DMA,
                pltpu.SemaphoreType.DMA,
                pltpu.SemaphoreType.DMA,
            ],
        ),
        compiler_params=pltpu.CompilerParams(vmem_limit_bytes=60 * 2**20),
        cost_estimate=pl.CostEstimate(flops=2 * tall * deep * wide, bytes_accessed=2**23, transcendentals=0),
        name="project_last",
    )(cols, *parts, weights, share)


def local(tokens, neighbor_bank, slots, w_query, w_key, w_value, w_out):
    blocks = neighbor_bank.shape[0]
    me, head_at = lax.axis_index("seq"), lax.axis_index("head")
    rows = origins(me)
    cols = jnp.stack([(head_at + d) % 4 for d in (0, 3, 1, 2)]).astype(jnp.int32)

    swap = [
        ((4 * a + j) * 4 + b, (4 * b + j) * 4 + a) for a in range(4) for b in range(4) for j in range(4)
    ]
    weights = (w_query, w_key, w_value)
    z_first = gather_z(pack(weights, 0, CHUNK_HEADS[0]))
    out_shard = lax.ppermute(w_out, ("seq", "head"), swap)
    normed, last = prepare(slots, neighbor_bank, tokens)

    x_first = gather_x(z_first)
    second = pack(weights, CHUNK_HEADS[0], CHUNK_HEADS[1], out_shard)
    z_second = gather_z(after(second, *z_first))
    devices = lax.axis_size("seq")
    arrived = lax.ppermute(last, "seq", [(i, i + 1) for i in range(devices - 1)])
    pieces = gather_core(x_first)

    block = tokens.shape[0] // blocks
    ring = lambda block, d: lax.ppermute(block, "head", [(i, (i + d) % 4) for i in range(4)])

    def exchange(own):
        return [own, ring(own, 1), ring(own, -1), ring(own, 2)]

    heads, x, own = CHUNK_HEADS[0], normed, None
    for n, (start, count) in enumerate(RUNS):
        own = attend(slots, rows, neighbor_bank, arrived, x, pieces, heads, start, count, GROUP, whole=True, into=own)
        x = after(normed, own)
        if n == 0:
            x_second = gather_x([after(p, own) for p in z_second])
    pieces = gather_core(x_second)
    first_parts = exchange(own)

    heads, runs = CHUNK_HEADS[1], []
    for n, (start, count) in enumerate(RUNS[::-1], 2):
        own = attend(slots, rows, neighbor_bank, arrived, x, pieces, heads, start, count, GROUP)
        x = after(normed, own)
        runs.append((start * block, exchange(own)))
    share, weights = project_first(rows, cols, first_parts, pieces, w_out.shape[0])
    return project_last(cols, runs, weights, share)


def solution(mesh):
    in_specs = (
        P(("batch", "seq"), None),
        P(("batch", "seq"), None, None),
        P(("batch", "seq")),
        P("seq", "head"),
        P("seq", "head"),
        P("seq", "head"),
        P("head", "seq"),
    )
    out_specs = P(("batch", "seq"), "head")

    return jax.shard_map(local, mesh=mesh, in_specs=in_specs, out_specs=out_specs, check_vma=False)
```

```python
import functools
import math

import jax
import jax.numpy as jnp
from jax import lax
from jax.experimental import pallas as pl
from jax.experimental.pallas import tpu as pltpu
from jax.sharding import PartitionSpec as P

HEAD_DIM = 128
X_LO, Z, CORE, X = 2, 4, 2, 4
CHUNK_HEADS = (2, 2)
RUNS = ((8, 8), (0, 8))
GROUP = 4
LAG = 2
AHEAD = 0
STAGES = {0: (0,), 1: (1, 2, 3)}


def route(move):
    pairs = []
    for x in range(X):
        for z in range(Z):
            for c in range(CORE):
                to_x, to_z, to_c = move(x, z, c)
                to_x, to_z, to_c = to_x % X, to_z % Z, to_c % CORE
                src = (((x % X_LO) * Z + z) * CORE + c) * 2 + x // X_LO
                dst = (((to_x % X_LO) * Z + to_z) * CORE + to_c) * 2 + to_x // X_LO
                pairs.append((src, dst))
    return pairs


Z_UP = route(lambda x, z, c: (x, z + 1, c))
Z_DOWN = route(lambda x, z, c: (x, z - 1, c))
Z_FAR = route(lambda x, z, c: (x, z + 2, c))
X_UP = route(lambda x, z, c: (x + 1, z, c))
X_DOWN = route(lambda x, z, c: (x - 1, z, c))
OTHER_CORE = route(lambda x, z, c: (x, z, c + 1))


def plane(block, pairs):
    return lax.ppermute(block, ("seq", "batch"), pairs)


def after(value, *earlier):
    return lax.optimization_barrier((value, *earlier))[0]


def gather_z(shard):
    return [shard, plane(shard, Z_UP), plane(shard, Z_DOWN), plane(shard, Z_FAR)]


def gather_x(around):
    near_pair, far_pair = jnp.stack(around[:2]), jnp.stack(around[2:])
    return [near_pair, far_pair, plane(near_pair, X_UP), plane(far_pair, X_DOWN)]


def gather_core(mine):
    near = [plane(p, OTHER_CORE) for p in mine[:2]]
    far = [plane(p, OTHER_CORE) for p in mine[2:]]
    return mine + near + far


def prepare_kernel(slots, bank, tokens, normed, last, sem):
    step = pl.program_id(0)

    @pl.when(step == 0)
    def _():
        pltpu.make_async_copy(bank.at[slots[bank.shape[0] - 1]], last, sem).start()

    hidden = tokens[...].astype(jnp.float32)
    scale = lax.rsqrt(jnp.mean(hidden * hidden, axis=-1, keepdims=True) + 1e-06)
    normed[...] = (hidden * scale).astype(jnp.bfloat16)

    @pl.when(step == pl.num_programs(0) - 1)
    def _():
        pltpu.make_async_copy(last, last, sem).wait()


def prepare(slots, bank, tokens):
    rows = pl.BlockSpec((tokens.shape[0] // 2, tokens.shape[1]), lambda i, *_: (i, 0))
    return pl.pallas_call(
        prepare_kernel,
        out_shape=(
            jax.ShapeDtypeStruct(tokens.shape, jnp.bfloat16),
            jax.ShapeDtypeStruct(bank.shape[1:], jnp.bfloat16),
        ),
        grid_spec=pltpu.PrefetchScalarGridSpec(
            num_scalar_prefetch=1,
            grid=(2,),
            in_specs=[pl.BlockSpec(memory_space=pl.ANY), rows],
            out_specs=[rows, pl.BlockSpec(bank.shape[1:], lambda i, *_: (0, 0))],
            scratch_shapes=[pltpu.SemaphoreType.DMA],
        ),
        cost_estimate=pl.CostEstimate(flops=2**30, bytes_accessed=2**23, transcendentals=0),
        name="prepare",
    )(slots, bank, tokens)


def pack_kernel(at, heads, *refs):
    ins, (out, sem) = refs[:-2], refs[-2:]
    for i in range(3):
        for h in range(heads):
            cols = pl.ds((at + h) * HEAD_DIM, HEAD_DIM)
            pltpu.make_async_copy(ins[i].at[:, cols], out.at[i * heads + h], sem).start()
    if len(ins) > 3:
        for i in range(out.shape[0] - 3 * heads):
            rows = pl.ds(i * HEAD_DIM, HEAD_DIM)
            pltpu.make_async_copy(ins[3].at[rows], out.at[3 * heads + i], sem).start()
    pltpu.make_async_copy(out, out, sem).wait()


def pack(weights, at, heads, *tail):
    count = 3 * heads + sum(t.shape[0] // HEAD_DIM for t in tail)
    return pl.pallas_call(
        functools.partial(pack_kernel, at, heads),
        out_shape=jax.ShapeDtypeStruct((count, weights[0].shape[0], HEAD_DIM), jnp.bfloat16),
        in_specs=[pl.BlockSpec(memory_space=pl.ANY)] * (3 + len(tail)),
        out_specs=pl.BlockSpec(memory_space=pltpu.VMEM),
        scratch_shapes=[pltpu.SemaphoreType.DMA],
        name="pack",
    )(*weights, *tail)


def origins():
    me = lax.axis_index("seq")
    x_lo, z, c = me // (Z * CORE), (me // CORE) % Z, me % CORE
    return [
        (x * Z + (z + dz) % Z) * CORE + core
        for core in (c, 1 - c)
        for x in (x_lo, 1 - x_lo)
        for dz in (0, 3, 1, 2)
    ]


def head_origins():
    me = lax.axis_index("head")
    return [(me + d) % 4 for d in (0, 3, 1, 2)]


def only_head(q, h, heads):
    empty = jnp.zeros((q.shape[0], HEAD_DIM), q.dtype)
    return jnp.concatenate(
        [q[:, i * HEAD_DIM : (i + 1) * HEAD_DIM] if i == h else empty for i in range(heads)], axis=1
    )


def attend_kernel(heads, first, group, slots, bank, normed, *rest):
    arrived, rest = (rest[0], rest[1:]) if first == 0 else (None, rest)
    pieces, out, ctx, w, x, ctx_sem, w_sem, x_sem = rest[:8], *rest[8:]
    step, steps = pl.program_id(0), pl.num_programs(0)
    width = heads * HEAD_DIM
    kv_rows = bank.shape[1]
    shard = pieces[0].shape[2]
    block = normed.shape[0] // bank.shape[0]
    tall = group * block

    def fetch_tokens(g, slot):
        at = pl.multiple_of(first * block + g * tall, tall)
        pltpu.make_async_copy(normed.at[pl.ds(at, tall)], x.at[slot], x_sem.at[slot]).start()

    def fetch(g, slot, j):
        c = first + g * group + j
        dst = ctx.at[slot, pl.ds(j * kv_rows, kv_rows), :]
        sem = ctx_sem.at[slot, j]
        if first == 0 and j == 0:

            @pl.when(g == 0)
            def _():
                pltpu.make_async_copy(arrived, dst, sem).start()

            @pl.when(g > 0)
            def _():
                pltpu.make_async_copy(bank.at[slots[jnp.maximum(c - 1, 0)]], dst, sem).start()
        else:
            pltpu.make_async_copy(bank.at[slots[c - 1]], dst, sem).start()

    def fetch_next():
        @pl.when(step + 1 < steps)
        def _():
            fetch_tokens(step + 1, (step + 1) % 2)
            for j in range(group):
                fetch(step + 1, (step + 1) % 2, j)

    @pl.when(step == 0)
    def _():
        rows = origins()
        for i in range(8):
            for k in range(2):
                at = pl.multiple_of(rows[i * 2 + k] * shard, shard)
                pltpu.make_async_copy(
                    pieces[i].at[k, pl.ds(0, 3 * heads)], w.at[:, pl.ds(at, shard), :], w_sem
                ).start()
        fetch_tokens(0, 0)
        fetch(0, 0, 0)

    slot = step % 2

    def compute(starting):
        if starting:
            pltpu.make_async_copy(w, w, w_sem).wait()
            for j in range(1, group):
                fetch(0, 0, j)
        else:
            fetch_next()
        pltpu.make_async_copy(x.at[slot], x.at[slot], x_sem.at[slot]).wait()
        blocks = [ctx.at[slot, pl.ds(j * kv_rows, kv_rows)] for j in range(group)]
        if not starting:
            for j in range(group):
                pltpu.make_async_copy(blocks[j], blocks[j], ctx_sem.at[slot, j]).wait()
        wq = jnp.concatenate([w[i] for i in range(heads)], axis=1)
        wkv = jnp.concatenate([w[i] for i in range(heads, 3 * heads)], axis=1)
        q = jnp.dot(x[slot], wq, preferred_element_type=jnp.float32).astype(jnp.bfloat16)
        kv, weights = {}, {}
        for j in range(group + 2 * LAG):
            if j < group:
                for k in STAGES.get(j, ()) if starting else ():
                    pltpu.make_async_copy(blocks[k], blocks[k], ctx_sem.at[slot, k]).wait()
                if starting and j == AHEAD:
                    fetch_next()
                kv[j] = jnp.dot(blocks[j][...], wkv, preferred_element_type=jnp.float32).astype(jnp.bfloat16)
            i = j - LAG
            if 0 <= i < group:
                qi = q[i * block : (i + 1) * block]
                stacked = jnp.concatenate([only_head(qi, h, heads) for h in range(heads)], axis=0)
                s = lax.dot_general(
                    stacked, kv[i][:, :width], (((1,), (1,)), ((), ())), preferred_element_type=jnp.float32
                )
                s = s * (1.0 / math.sqrt(HEAD_DIM))
                e = jnp.exp(s - jnp.max(s, axis=-1, keepdims=True))
                weights[i] = (e / jnp.sum(e, axis=-1, keepdims=True)).astype(jnp.bfloat16)
            i = j - 2 * LAG
            if 0 <= i < group:
                o = jnp.dot(weights[i], kv[i][:, width:], preferred_element_type=jnp.float32).astype(jnp.bfloat16)
                for h in range(heads):
                    cols = slice(h * HEAD_DIM, (h + 1) * HEAD_DIM)
                    out[i * block : (i + 1) * block, cols] = o[h * block : (h + 1) * block, cols]

    @pl.when(step == 0)
    def _():
        compute(True)

    @pl.when(step > 0)
    def _():
        compute(False)


def attend(slots, bank, arrived, normed, pieces, heads, first, blocks, group):
    model = normed.shape[1]
    kv_rows = bank.shape[1]
    arrived = [arrived] if first == 0 else []
    block = normed.shape[0] // bank.shape[0]
    width = heads * HEAD_DIM
    hbm = pl.BlockSpec(memory_space=pltpu.HBM)
    flops = 2 * blocks * (2 * kv_rows + block) * model * width
    return pl.pallas_call(
        functools.partial(attend_kernel, heads, first, group),
        out_shape=jax.ShapeDtypeStruct((blocks * block, width), jnp.bfloat16),
        grid_spec=pltpu.PrefetchScalarGridSpec(
            num_scalar_prefetch=1,
            grid=(blocks // group,),
            in_specs=[hbm] * (2 + len(arrived) + 8),
            out_specs=pl.BlockSpec((group * block, width), lambda i, *_: (i, 0)),
            scratch_shapes=[
                pltpu.VMEM((2, group * kv_rows, model), jnp.bfloat16),
                pltpu.VMEM((3 * heads, model, HEAD_DIM), jnp.bfloat16),
                pltpu.VMEM((2, group * block, model), jnp.bfloat16),
                pltpu.SemaphoreType.DMA((2, group)),
                pltpu.SemaphoreType.DMA,
                pltpu.SemaphoreType.DMA((2,)),
            ],
        ),
        cost_estimate=pl.CostEstimate(
            flops=flops, bytes_accessed=2 * blocks * kv_rows * model, transcendentals=0
        ),
        compiler_params=pltpu.CompilerParams(vmem_limit_bytes=60 * 2**20),
        name="attend",
    )(slots, bank, normed, *arrived, *pieces)


def load_parts(parts, att, sem):
    width = parts[0].shape[1]
    for part, origin in zip(parts, head_origins()):
        pltpu.make_async_copy(part, att.at[:, pl.ds(pl.multiple_of(origin * width, width), width)], sem).start()


def project_first_kernel(*refs):
    parts, pieces = refs[:12], refs[12:20]
    out, share, w_next, w, att, att_sem, w_sem, next_sem = refs[20:]
    deep, wide = w.shape[0] // 4, w.shape[1] // 4
    tile = pieces[0].shape[2]
    count = deep // tile
    lead = pieces[0].shape[1] - 2 * count
    rows = origins()
    for i in range(2):
        load_parts(parts[4 * i : 4 * i + 4], att.at[i], att_sem.at[i])
    for dst, sem, at in ((w, w_sem, lead), (w_next, next_sem, lead + count)):
        for i in range(8):
            for k in range(2):
                r = pl.multiple_of((rows[i * 2 + k] // 4) * deep, deep)
                c = pl.multiple_of((rows[i * 2 + k] % 4) * wide, wide)
                for t in range(count):
                    pltpu.make_async_copy(
                        pieces[i].at[k, at + t], dst.at[pl.ds(r + t * tile, tile), pl.ds(c, wide)], sem
                    ).start()
    load_parts(parts[8:], att.at[2], att_sem.at[2])
    for i in range(2):
        pltpu.make_async_copy(att.at[i], att.at[i], att_sem.at[i]).wait()
    pltpu.make_async_copy(w, w, w_sem).wait()
    share[...] = jnp.dot(att[1], w[...], preferred_element_type=jnp.float32)
    begun = jnp.dot(att[0], w[...], preferred_element_type=jnp.float32)
    pltpu.make_async_copy(w_next, w_next, next_sem).wait()
    pltpu.make_async_copy(att.at[2], att.at[2], att_sem.at[2]).wait()
    rest = jnp.dot(att[2], w_next[...], preferred_element_type=jnp.float32)
    out[...] = (begun + rest).astype(jnp.bfloat16)


def project_first(early, late, first, second, pieces, tall, wide):
    rows, width = first[early][0].shape
    deep = 4 * width
    hbm = pl.BlockSpec(memory_space=pltpu.HBM)
    parts = [*first[early], *first[late], *second[early]]
    at = early[0] // early[1]
    return pl.pallas_call(
        project_first_kernel,
        out_shape=(
            jax.ShapeDtypeStruct((tall, wide), jnp.bfloat16),
            jax.ShapeDtypeStruct((rows, wide), jnp.float32),
            jax.ShapeDtypeStruct((deep, wide), jnp.bfloat16),
        ),
        grid=(1,),
        in_specs=[hbm] * (len(parts) + 8),
        out_specs=(
            pl.BlockSpec((rows, wide), lambda i: (at, 0)),
            pl.BlockSpec((rows, wide), lambda i: (0, 0)),
            pl.BlockSpec((deep, wide), lambda i: (0, 0)),
        ),
        scratch_shapes=[
            pltpu.VMEM((deep, wide), jnp.bfloat16),
            pltpu.VMEM((3, rows, deep), jnp.bfloat16),
            pltpu.SemaphoreType.DMA((3,)),
            pltpu.SemaphoreType.DMA,
            pltpu.SemaphoreType.DMA,
        ],
        compiler_params=pltpu.CompilerParams(vmem_limit_bytes=60 * 2**20),
        cost_estimate=pl.CostEstimate(flops=2 * tall * deep * wide, bytes_accessed=2**23, transcendentals=0),
        name="project_first",
    )(*parts, *pieces)


def project_last_kernel(*refs):
    parts, (w_in, share_in, _, out, w, share, att, w_sem, sem, att_sem) = refs[:4], refs[4:]
    load_parts(parts, att, att_sem)
    pltpu.make_async_copy(w_in, w, w_sem).start()
    pltpu.make_async_copy(share_in, share, sem).start()
    pltpu.make_async_copy(att, att, att_sem).wait()
    pltpu.make_async_copy(w, w, w_sem).wait()
    pltpu.make_async_copy(share, share, sem).wait()
    rest = jnp.dot(att[...], w[...], preferred_element_type=jnp.float32)
    out[...] = (share[...] + rest).astype(jnp.bfloat16)


def project_last(late, parts, weights, share, out):
    (rows, wide), deep = share.shape, weights.shape[0]
    hbm = pl.BlockSpec(memory_space=pltpu.HBM)
    at = late[0] // late[1]
    return pl.pallas_call(
        project_last_kernel,
        out_shape=jax.ShapeDtypeStruct(out.shape, out.dtype),
        grid=(1,),
        in_specs=[hbm] * 7,
        out_specs=pl.BlockSpec((rows, wide), lambda i: (at, 0)),
        scratch_shapes=[
            pltpu.VMEM((deep, wide), jnp.bfloat16),
            pltpu.VMEM((rows, wide), jnp.float32),
            pltpu.VMEM((rows, deep), jnp.bfloat16),
            pltpu.SemaphoreType.DMA,
            pltpu.SemaphoreType.DMA,
            pltpu.SemaphoreType.DMA,
        ],
        input_output_aliases={6: 0},
        compiler_params=pltpu.CompilerParams(vmem_limit_bytes=60 * 2**20),
        cost_estimate=pl.CostEstimate(flops=2 * rows * deep * wide, bytes_accessed=2**22, transcendentals=0),
        name="project_last",
    )(*parts, weights, share, out)


def local(tokens, neighbor_bank, slots, w_query, w_key, w_value, w_out):
    swap = [
        ((4 * a + j) * 4 + b, (4 * b + j) * 4 + a) for a in range(4) for b in range(4) for j in range(4)
    ]
    weights = (w_query, w_key, w_value)
    z_first = gather_z(pack(weights, 0, CHUNK_HEADS[0]))
    out_shard = lax.ppermute(w_out, ("seq", "head"), swap)
    normed, last = prepare(slots, neighbor_bank, tokens)

    x_first = gather_x(z_first)
    second = pack(weights, CHUNK_HEADS[0], CHUNK_HEADS[1], out_shard)
    z_second = gather_z(after(second, *z_first))
    devices = lax.axis_size("seq")
    arrived = lax.ppermute(last, "seq", [(i, i + 1) for i in range(devices - 1)])
    pieces = gather_core(x_first)

    ring = lambda block, d: lax.ppermute(block, "head", [(i, (i + d) % 4) for i in range(4)])

    def exchange(own):
        return [own, ring(own, 1), ring(own, -1), ring(own, 2)]

    x, chunks, n = normed, [], 0
    for heads, order in zip(CHUNK_HEADS, (RUNS, RUNS[::-1])):
        runs = {}
        for start, count in order:
            own = attend(slots, neighbor_bank, arrived, x, pieces, heads, start, count, GROUP)
            x = after(normed, own)
            runs[start, count] = exchange(own)
            if n == 0:
                x_second = gather_x([after(p, own) for p in z_second])
            if n == 1:
                pieces = gather_core(x_second)
            n += 1
        chunks.append(runs)
    late, early = RUNS
    out, share, weights = project_first(early, late, *chunks, pieces, tokens.shape[0], w_out.shape[0])
    return project_last(late, chunks[1][late], weights, share, out)


def solution(mesh):
    in_specs = (
        P(("batch", "seq"), None),
        P(("batch", "seq"), None, None),
        P(("batch", "seq")),
        P("seq", "head"),
        P("seq", "head"),
        P("seq", "head"),
        P("head", "seq"),
    )
    out_specs = P(("batch", "seq"), "head")

    return jax.shard_map(local, mesh=mesh, in_specs=in_specs, out_specs=out_specs, check_vma=False)
```

```python
import functools
import math

import jax
import jax.numpy as jnp
from jax import lax
from jax.experimental import pallas as pl
from jax.experimental.pallas import tpu as pltpu
from jax.sharding import PartitionSpec as P

HEAD_DIM = 128
X_LO, Z, CORE, X = 2, 4, 2, 4
CHUNK_HEADS = (2, 2)
RUNS = (((8, 8), (0, 8)), ((0, 8), (8, 8)))
GROUP = 4
LAG = 2
AHEAD = 0
STAGES = {0: (0,), 1: (1, 2, 3)}


def route(move):
    pairs = []
    for x in range(X):
        for z in range(Z):
            for c in range(CORE):
                to_x, to_z, to_c = move(x, z, c)
                to_x, to_z, to_c = to_x % X, to_z % Z, to_c % CORE
                src = (((x % X_LO) * Z + z) * CORE + c) * 2 + x // X_LO
                dst = (((to_x % X_LO) * Z + to_z) * CORE + to_c) * 2 + to_x // X_LO
                pairs.append((src, dst))
    return pairs


Z_UP = route(lambda x, z, c: (x, z + 1, c))
Z_DOWN = route(lambda x, z, c: (x, z - 1, c))
Z_FAR = route(lambda x, z, c: (x, z + 2, c))
X_UP = route(lambda x, z, c: (x + 1, z, c))
X_DOWN = route(lambda x, z, c: (x - 1, z, c))
OTHER_CORE = route(lambda x, z, c: (x, z, c + 1))


def plane(block, pairs):
    return lax.ppermute(block, ("seq", "batch"), pairs)


def after(value, *earlier):
    return lax.optimization_barrier((value, *earlier))[0]


def gather_z(shard):
    return [shard, plane(shard, Z_UP), plane(shard, Z_DOWN), plane(shard, Z_FAR)]


def gather_x(around):
    near_pair, far_pair = jnp.stack(around[:2]), jnp.stack(around[2:])
    return [near_pair, far_pair, plane(near_pair, X_UP), plane(far_pair, X_DOWN)]


def gather_core(mine):
    near = [plane(p, OTHER_CORE) for p in mine[:2]]
    far = [plane(p, OTHER_CORE) for p in mine[2:]]
    return mine + near + far


def prepare_kernel(slots, bank, tokens, normed, last, sem):
    step = pl.program_id(0)

    @pl.when(step == 0)
    def _():
        pltpu.make_async_copy(bank.at[slots[bank.shape[0] - 1]], last, sem).start()

    hidden = tokens[...].astype(jnp.float32)
    scale = lax.rsqrt(jnp.mean(hidden * hidden, axis=-1, keepdims=True) + 1e-06)
    normed[...] = (hidden * scale).astype(jnp.bfloat16)

    @pl.when(step == pl.num_programs(0) - 1)
    def _():
        pltpu.make_async_copy(last, last, sem).wait()


def prepare(slots, bank, tokens):
    rows = pl.BlockSpec((tokens.shape[0] // 2, tokens.shape[1]), lambda i, *_: (i, 0))
    return pl.pallas_call(
        prepare_kernel,
        out_shape=(
            jax.ShapeDtypeStruct(tokens.shape, jnp.bfloat16),
            jax.ShapeDtypeStruct(bank.shape[1:], jnp.bfloat16),
        ),
        grid_spec=pltpu.PrefetchScalarGridSpec(
            num_scalar_prefetch=1,
            grid=(2,),
            in_specs=[pl.BlockSpec(memory_space=pl.ANY), rows],
            out_specs=[rows, pl.BlockSpec(bank.shape[1:], lambda i, *_: (0, 0))],
            scratch_shapes=[pltpu.SemaphoreType.DMA],
        ),
        cost_estimate=pl.CostEstimate(flops=2**30, bytes_accessed=2**23, transcendentals=0),
        name="prepare",
    )(slots, bank, tokens)


def pack_kernel(at, heads, *refs):
    ins, (out, sem) = refs[:-2], refs[-2:]
    for i in range(3):
        for h in range(heads):
            cols = pl.ds((at + h) * HEAD_DIM, HEAD_DIM)
            pltpu.make_async_copy(ins[i].at[:, cols], out.at[i * heads + h], sem).start()
    if len(ins) > 3:
        for i in range(out.shape[0] - 3 * heads):
            rows = pl.ds(i * HEAD_DIM, HEAD_DIM)
            pltpu.make_async_copy(ins[3].at[rows], out.at[3 * heads + i], sem).start()
    pltpu.make_async_copy(out, out, sem).wait()


def pack(weights, at, heads, *tail):
    count = 3 * heads + sum(t.shape[0] // HEAD_DIM for t in tail)
    return pl.pallas_call(
        functools.partial(pack_kernel, at, heads),
        out_shape=jax.ShapeDtypeStruct((count, weights[0].shape[0], HEAD_DIM), jnp.bfloat16),
        in_specs=[pl.BlockSpec(memory_space=pl.ANY)] * (3 + len(tail)),
        out_specs=pl.BlockSpec(memory_space=pltpu.VMEM),
        scratch_shapes=[pltpu.SemaphoreType.DMA],
        name="pack",
    )(*weights, *tail)


def origins():
    me = lax.axis_index("seq")
    x_lo, z, c = me // (Z * CORE), (me // CORE) % Z, me % CORE
    return [
        (x * Z + (z + dz) % Z) * CORE + core
        for core in (c, 1 - c)
        for x in (x_lo, 1 - x_lo)
        for dz in (0, 3, 1, 2)
    ]


def head_origins():
    me = lax.axis_index("head")
    return [(me + d) % 4 for d in (0, 3, 1, 2)]


def only_head(q, h, heads):
    empty = jnp.zeros((q.shape[0], HEAD_DIM), q.dtype)
    return jnp.concatenate(
        [q[:, i * HEAD_DIM : (i + 1) * HEAD_DIM] if i == h else empty for i in range(heads)], axis=1
    )


def attend_kernel(heads, first, group, slots, bank, normed, *rest):
    arrived, rest = (rest[0], rest[1:]) if first == 0 else (None, rest)
    pieces, out, ctx, w, x, ctx_sem, w_sem, x_sem = rest[:8], *rest[8:]
    step, steps = pl.program_id(0), pl.num_programs(0)
    width = heads * HEAD_DIM
    kv_rows = bank.shape[1]
    shard = pieces[0].shape[2]
    block = normed.shape[0] // bank.shape[0]
    tall = group * block

    def fetch_tokens(g, slot):
        at = pl.multiple_of(first * block + g * tall, tall)
        pltpu.make_async_copy(normed.at[pl.ds(at, tall)], x.at[slot], x_sem.at[slot]).start()

    def fetch(g, slot, j):
        c = first + g * group + j
        dst = ctx.at[slot, pl.ds(j * kv_rows, kv_rows), :]
        sem = ctx_sem.at[slot, j]
        if first == 0 and j == 0:

            @pl.when(g == 0)
            def _():
                pltpu.make_async_copy(arrived, dst, sem).start()

            @pl.when(g > 0)
            def _():
                pltpu.make_async_copy(bank.at[slots[jnp.maximum(c - 1, 0)]], dst, sem).start()
        else:
            pltpu.make_async_copy(bank.at[slots[c - 1]], dst, sem).start()

    def fetch_next():
        @pl.when(step + 1 < steps)
        def _():
            fetch_tokens(step + 1, (step + 1) % 2)
            for j in range(group):
                fetch(step + 1, (step + 1) % 2, j)

    @pl.when(step == 0)
    def _():
        rows = origins()
        for i in range(8):
            for k in range(2):
                at = pl.multiple_of(rows[i * 2 + k] * shard, shard)
                pltpu.make_async_copy(
                    pieces[i].at[k, pl.ds(0, 3 * heads)], w.at[:, pl.ds(at, shard), :], w_sem
                ).start()
        fetch_tokens(0, 0)
        fetch(0, 0, 0)

    slot = step % 2

    def compute(starting):
        if starting:
            pltpu.make_async_copy(w, w, w_sem).wait()
            for j in range(1, group):
                fetch(0, 0, j)
        else:
            fetch_next()
        pltpu.make_async_copy(x.at[slot], x.at[slot], x_sem.at[slot]).wait()
        blocks = [ctx.at[slot, pl.ds(j * kv_rows, kv_rows)] for j in range(group)]
        if not starting:
            for j in range(group):
                pltpu.make_async_copy(blocks[j], blocks[j], ctx_sem.at[slot, j]).wait()
        wq = jnp.concatenate([w[i] for i in range(heads)], axis=1)
        wkv = jnp.concatenate([w[i] for i in range(heads, 3 * heads)], axis=1)
        q = jnp.dot(x[slot], wq, preferred_element_type=jnp.float32).astype(jnp.bfloat16)
        kv, weights = {}, {}
        for j in range(group + 2 * LAG):
            if j < group:
                for k in STAGES.get(j, ()) if starting else ():
                    pltpu.make_async_copy(blocks[k], blocks[k], ctx_sem.at[slot, k]).wait()
                if starting and j == AHEAD:
                    fetch_next()
                kv[j] = jnp.dot(blocks[j][...], wkv, preferred_element_type=jnp.float32).astype(jnp.bfloat16)
            i = j - LAG
            if 0 <= i < group:
                qi = q[i * block : (i + 1) * block]
                stacked = jnp.concatenate([only_head(qi, h, heads) for h in range(heads)], axis=0)
                s = lax.dot_general(
                    stacked, kv[i][:, :width], (((1,), (1,)), ((), ())), preferred_element_type=jnp.float32
                )
                s = s * (1.0 / math.sqrt(HEAD_DIM))
                e = jnp.exp(s - jnp.max(s, axis=-1, keepdims=True))
                weights[i] = (e / jnp.sum(e, axis=-1, keepdims=True)).astype(jnp.bfloat16)
            i = j - 2 * LAG
            if 0 <= i < group:
                o = jnp.dot(weights[i], kv[i][:, width:], preferred_element_type=jnp.float32).astype(jnp.bfloat16)
                for h in range(heads):
                    cols = slice(h * HEAD_DIM, (h + 1) * HEAD_DIM)
                    out[i * block : (i + 1) * block, cols] = o[h * block : (h + 1) * block, cols]

    @pl.when(step == 0)
    def _():
        compute(True)

    @pl.when(step > 0)
    def _():
        compute(False)


def attend(slots, bank, arrived, normed, pieces, heads, first, blocks, group):
    model = normed.shape[1]
    kv_rows = bank.shape[1]
    arrived = [arrived] if first == 0 else []
    block = normed.shape[0] // bank.shape[0]
    width = heads * HEAD_DIM
    hbm = pl.BlockSpec(memory_space=pl.ANY)
    flops = 2 * blocks * (2 * kv_rows + block) * model * width
    return pl.pallas_call(
        functools.partial(attend_kernel, heads, first, group),
        out_shape=jax.ShapeDtypeStruct((blocks * block, width), jnp.bfloat16),
        grid_spec=pltpu.PrefetchScalarGridSpec(
            num_scalar_prefetch=1,
            grid=(blocks // group,),
            in_specs=[hbm] * (2 + len(arrived) + 8),
            out_specs=pl.BlockSpec((group * block, width), lambda i, *_: (i, 0)),
            scratch_shapes=[
                pltpu.VMEM((2, group * kv_rows, model), jnp.bfloat16),
                pltpu.VMEM((3 * heads, model, HEAD_DIM), jnp.bfloat16),
                pltpu.VMEM((2, group * block, model), jnp.bfloat16),
                pltpu.SemaphoreType.DMA((2, group)),
                pltpu.SemaphoreType.DMA,
                pltpu.SemaphoreType.DMA((2,)),
            ],
        ),
        cost_estimate=pl.CostEstimate(
            flops=flops, bytes_accessed=2 * blocks * kv_rows * model, transcendentals=0
        ),
        compiler_params=pltpu.CompilerParams(vmem_limit_bytes=24 * 2**20),
        name="attend",
    )(slots, bank, normed, *arrived, *pieces)


def load_parts(parts, att, sem):
    width = parts[0].shape[1]
    for part, origin in zip(parts, head_origins()):
        pltpu.make_async_copy(part, att.at[:, pl.ds(pl.multiple_of(origin * width, width), width)], sem).start()


def project_first_kernel(starts, *refs):
    n = 4 * len(starts)
    parts, early, pieces = refs[:n], refs[n : n + 4], refs[n + 4 : n + 12]
    out, share, w_next, w, att, att_next, att_sem, att_next_sem, w_sem, next_sem = refs[n + 12 :]
    deep, wide = w.shape[0] // 4, w.shape[1] // 4
    tile = pieces[0].shape[2]
    count = deep // tile
    lead = pieces[0].shape[1] - 2 * count
    rows = origins()
    for i, start in enumerate(starts):
        four = parts[4 * i : 4 * i + 4]
        load_parts(four, att.at[pl.ds(start, four[0].shape[0])], att_sem)
    for dst, sem, at in ((w, w_sem, lead), (w_next, next_sem, lead + count)):
        for i in range(8):
            for k in range(2):
                r = pl.multiple_of((rows[i * 2 + k] // 4) * deep, deep)
                c = pl.multiple_of((rows[i * 2 + k] % 4) * wide, wide)
                for t in range(count):
                    pltpu.make_async_copy(
                        pieces[i].at[k, at + t], dst.at[pl.ds(r + t * tile, tile), pl.ds(c, wide)], sem
                    ).start()
    load_parts(early, att_next, att_next_sem)
    pltpu.make_async_copy(att, att, att_sem).wait()
    pltpu.make_async_copy(w, w, w_sem).wait()
    tall = out.shape[0]
    share[...] = jnp.dot(att[tall:], w[...], preferred_element_type=jnp.float32)
    begun = jnp.dot(att[:tall], w[...], preferred_element_type=jnp.float32)
    pltpu.make_async_copy(w_next, w_next, next_sem).wait()
    pltpu.make_async_copy(att_next, att_next, att_next_sem).wait()
    rest = jnp.dot(att_next[...], w_next[...], preferred_element_type=jnp.float32)
    out[...] = (begun + rest).astype(jnp.bfloat16)


def project_first(first, early, pieces, tall, wide):
    rows, width = early[0].shape
    deep = 4 * width
    hbm, anywhere = pl.BlockSpec(memory_space=pltpu.HBM), pl.BlockSpec(memory_space=pl.ANY)
    starts = tuple(start for start, _ in first)
    parts = [p for _, four in first for p in four] + early
    return pl.pallas_call(
        functools.partial(project_first_kernel, starts),
        out_shape=(
            jax.ShapeDtypeStruct((tall, wide), jnp.bfloat16),
            jax.ShapeDtypeStruct((tall - rows, wide), jnp.float32),
            jax.ShapeDtypeStruct((deep, wide), jnp.bfloat16),
        ),
        grid=(1,),
        in_specs=[anywhere] * (len(parts) + 8),
        out_specs=(
            pl.BlockSpec((rows, wide), lambda i: (0, 0)),
            pl.BlockSpec((tall - rows, wide), lambda i: (0, 0)),
            pl.BlockSpec((deep, wide), lambda i: (0, 0)),
        ),
        scratch_shapes=[
            pltpu.VMEM((deep, wide), jnp.bfloat16),
            pltpu.VMEM((tall, deep), jnp.bfloat16),
            pltpu.VMEM((rows, deep), jnp.bfloat16),
            pltpu.SemaphoreType.DMA,
            pltpu.SemaphoreType.DMA,
            pltpu.SemaphoreType.DMA,
            pltpu.SemaphoreType.DMA,
        ],
        compiler_params=pltpu.CompilerParams(vmem_limit_bytes=20 * 2**20),
        cost_estimate=pl.CostEstimate(flops=2 * tall * deep * wide, bytes_accessed=2**23, transcendentals=0),
        name="project_first",
    )(*parts, *pieces)


def project_last_kernel(*refs):
    parts, (w_in, share_in, _, out, w, share, att, w_sem, sem, att_sem) = refs[:4], refs[4:]
    load_parts(parts, att, att_sem)
    pltpu.make_async_copy(w_in, w, w_sem).start()
    pltpu.make_async_copy(share_in, share, sem).start()
    pltpu.make_async_copy(att, att, att_sem).wait()
    pltpu.make_async_copy(w, w, w_sem).wait()
    pltpu.make_async_copy(share, share, sem).wait()
    rest = jnp.dot(att[...], w[...], preferred_element_type=jnp.float32)
    out[...] = (share[...] + rest).astype(jnp.bfloat16)


def project_last(parts, weights, share, out):
    (rows, wide), deep = share.shape, weights.shape[0]
    anywhere = pl.BlockSpec(memory_space=pl.ANY)
    at = out.shape[0] // rows - 1
    return pl.pallas_call(
        project_last_kernel,
        out_shape=jax.ShapeDtypeStruct(out.shape, out.dtype),
        grid=(1,),
        in_specs=[anywhere] * 7,
        out_specs=pl.BlockSpec((rows, wide), lambda i: (at, 0)),
        scratch_shapes=[
            pltpu.VMEM((deep, wide), jnp.bfloat16),
            pltpu.VMEM((rows, wide), jnp.float32),
            pltpu.VMEM((rows, deep), jnp.bfloat16),
            pltpu.SemaphoreType.DMA,
            pltpu.SemaphoreType.DMA,
            pltpu.SemaphoreType.DMA,
        ],
        input_output_aliases={6: 0},
        compiler_params=pltpu.CompilerParams(vmem_limit_bytes=16 * 2**20),
        cost_estimate=pl.CostEstimate(flops=2 * rows * deep * wide, bytes_accessed=2**22, transcendentals=0),
        name="project_last",
    )(*parts, weights, share, out)


def local(tokens, neighbor_bank, slots, w_query, w_key, w_value, w_out):
    blocks = neighbor_bank.shape[0]
    swap = [
        ((4 * a + j) * 4 + b, (4 * b + j) * 4 + a) for a in range(4) for b in range(4) for j in range(4)
    ]
    weights = (w_query, w_key, w_value)
    z_first = gather_z(pack(weights, 0, CHUNK_HEADS[0]))
    out_shard = lax.ppermute(w_out, ("seq", "head"), swap)
    normed, last = prepare(slots, neighbor_bank, tokens)

    x_first = gather_x(z_first)
    second = pack(weights, CHUNK_HEADS[0], CHUNK_HEADS[1], out_shard)
    z_second = gather_z(after(second, *z_first))
    devices = lax.axis_size("seq")
    arrived = lax.ppermute(last, "seq", [(i, i + 1) for i in range(devices - 1)])
    pieces = gather_core(x_first)

    ring = lambda block, d: lax.ppermute(block, "head", [(i, (i + d) % 4) for i in range(4)])

    def exchange(own):
        return [own, ring(own, 1), ring(own, -1), ring(own, 2)]

    x, chunks, n = normed, [], 0
    for heads, order in zip(CHUNK_HEADS, RUNS):
        runs = []
        for start, count in order:
            own = attend(slots, neighbor_bank, arrived, x, pieces, heads, start, count, GROUP)
            x = after(normed, own)
            runs.append((start * tokens.shape[0] // blocks, exchange(own)))
            if n == 0:
                x_second = gather_x([after(p, own) for p in z_second])
            if n == 1:
                pieces = gather_core(x_second)
            n += 1
        chunks.append(runs)
    (_, early), (_, late) = chunks[1]
    out, share, weights = project_first(chunks[0], early, pieces, tokens.shape[0], w_out.shape[0])
    return project_last(late, weights, share, out)


def solution(mesh):
    in_specs = (
        P(("batch", "seq"), None),
        P(("batch", "seq"), None, None),
        P(("batch", "seq")),
        P("seq", "head"),
        P("seq", "head"),
        P("seq", "head"),
        P("head", "seq"),
    )
    out_specs = P(("batch", "seq"), "head")

    return jax.shard_map(local, mesh=mesh, in_specs=in_specs, out_specs=out_specs, check_vma=False)
```
